32 devices in a mesh: ep: 4 (over y, x), tp: 4 (over z), dp: 2 (over core).
Axes of the slice: x: 2, y: 2, z: 4, core: 2. Of those that a mesh axis runs over, the one named last changes fastest.
Arguments:
- down_weight: bfloat16 [4, 16384, 3072], P('ep', 'tp', 'dp'), may hold values from -130 to 130
- owned_span: int32 [4, 4, 2], replicated, may hold values from 0 to 31, as said below
Outputs:
- saved_spans: bfloat16 [4, 4, 768, 16384], P('ep', 'tp', 'dp')
The draws below stay inside these ranges and needn't reach their ends.
Inputs may be any that keep to these rules, and one draw needn't show every extreme that they name: `owned_span`: block g holds rows (g % 8) * 384 onward of expert g // 8; every block is stored by exactly one device; the block at [i, j, k] has (g % 8) // 4 == k; for each k the experts of the stored blocks form a Latin square over i and j: each expert once for each i and once for each j.
All inputs are finite; a program needn't handle non-finite values.
Results may differ from the reference program's by a relative error of at most 0.001.
Values may be sent and summed in bfloat16 or wider, within the bound.
A program may use at most 128 MiB of HBM per device.

```python
import jax
import jax.numpy as jnp

FF = 16384
EXPERTS = 4
SLAB = 3072
BLOCK_ROWS = 384
N_EP = 4
N_TP = 4
N_DP = 2


def permuted_rows(key, count_rows, width):
    scores = jax.random.randint(key, (count_rows, width), 0, 1 << 20) * width + jnp.arange(width, dtype=jnp.int32)[None, :]
    return jnp.argsort(scores, axis=1).astype(jnp.int32)


def draw_owned_span(key, part):
    key_list = jax.random.split(jax.random.fold_in(key, 23), 4)
    per_expert = N_TP * N_DP
    row_perm = permuted_rows(key_list[0], N_DP, N_EP)
    col_perm = permuted_rows(key_list[1], N_DP, N_TP)
    relabel = permuted_rows(key_list[2], N_DP, N_EP)
    block_perm = permuted_rows(key_list[3], N_DP * N_EP, N_TP).reshape(N_DP, N_EP, N_TP)
    summed = (row_perm[:, :, None] + col_perm[:, None, :]) % N_EP
    latin_square = jnp.take_along_axis(relabel[:, :, None], summed.reshape(N_DP, N_EP * N_TP, 1), axis=1).reshape(N_DP, N_EP, N_TP)
    replica_ids = jnp.arange(N_DP, dtype=jnp.int32)[:, None, None] + jnp.zeros((N_DP, N_EP, N_TP), jnp.int32)
    ep_ids = jnp.arange(N_EP, dtype=jnp.int32)[None, :, None] + jnp.zeros((N_DP, N_EP, N_TP), jnp.int32)
    within = replica_ids * N_TP + block_perm[replica_ids, latin_square, ep_ids]
    global_ids = latin_square * per_expert + within
    return jnp.transpose(global_ids, (1, 2, 0)).astype(jnp.int32)


def draw_down_weight(key, part):
    key_list = jax.random.split(jax.random.fold_in(key, 11), 3)
    base_draw = jnp.clip(jax.random.normal(key_list[0], (EXPERTS, FF, SLAB), jnp.float32), -4.0, 4.0)
    spread = 1.15
    row_scale = jnp.exp(jax.random.uniform(key_list[1], (SLAB,), jnp.float32, -spread, spread))
    col_scale = jnp.exp(jax.random.uniform(key_list[2], (FF,), jnp.float32, -spread, spread))
    expert_scale = jnp.power(3.0, jnp.arange(EXPERTS, dtype=jnp.float32) / max(EXPERTS - 1, 1))
    values = base_draw * expert_scale[:, None, None] * col_scale[None, :, None] * row_scale[None, None, :]
    return values.astype(jnp.bfloat16)


def setup_inputs(seed: int = 0) -> dict:
    keys = jax.random.split(jax.random.key(seed), 3)
    down_weight = draw_down_weight(jax.random.fold_in(keys[2], 71), 0)
    owned_span = draw_owned_span(jax.random.fold_in(keys[2], 71), 0)
    return {"down_weight": down_weight, "owned_span": owned_span}


def reference(down_weight, owned_span):
    per_expert = N_TP * N_DP
    saved_rows = jnp.transpose(down_weight, (0, 2, 1)).reshape(EXPERTS * per_expert, BLOCK_ROWS, FF)
    owner_list = owned_span.reshape(-1).astype(jnp.int32)
    picked = jnp.take(saved_rows, owner_list, axis=0)
    saved_spans = picked.reshape(N_EP, N_TP, N_DP * BLOCK_ROWS, FF)
    return saved_spans
```

```python
import functools

import jax
import jax.numpy as jnp
from jax import lax
from jax.experimental import pallas as pl
from jax.experimental.pallas import tpu as pltpu
from jax.sharding import PartitionSpec as P

MESH = pl.DeviceIdType.MESH
LANES = 128
SUBLANES = 16
CHUNK = 256
STAGES = 4
AHEAD = 2
SPARE = 3 << 20
WRITES = 8


def pick(values, index):
    chosen = values[0]
    for b in range(1, len(values)):
        chosen = jnp.where(index == b, values[b], chosen)
    return chosen


def kernel(n_ep, n_tp, n_dp, chunk, weight, span_hbm, out, stage, turned, send, relay, span,
           load_sem, span_sem, ep_send, ep_recv, tp_send, tp_recv, own_sem, early, middle, spread, late,
           early_send, early_recv, fan_send, fan_recv, late_sem, *arrived):
    my_ep = lax.axis_index("ep")
    my_tp = lax.axis_index("tp")
    my_dp = lax.axis_index("dp")
    hidden, width = weight.shape[1], weight.shape[2]
    rows = width // n_tp
    chunks = hidden // chunk
    per_expert = n_tp * n_dp

    def load(c):
        return pltpu.make_async_copy(
            weight.at[0, pl.ds(c * chunk, chunk)], stage.at[c % STAGES], load_sem.at[c % STAGES])

    def to_ep(c, d):
        return pltpu.make_async_remote_copy(
            send.at[c, d], arrived[c - 1].at[d], ep_send.at[c, d], ep_recv.at[c, d],
            device_id={"ep": lax.rem(my_ep + d, n_ep)}, device_id_type=MESH)

    def columns(tp, c):
        return out.at[0, 0, :, pl.ds(pl.multiple_of(tp * hidden + c * chunk, chunk), chunk)]

    def to_tp(c, d):
        return pltpu.make_async_remote_copy(
            relay.at[c, d], columns(my_tp, c), tp_send.at[c, d], tp_recv.at[c, d],
            device_id={"tp": lax.rem(my_tp + d, n_tp)}, device_id_type=MESH)

    def from_tp(c, d):
        return pltpu.make_async_remote_copy(
            relay.at[c, d], columns(lax.rem(my_tp + n_tp - d, n_tp), c), tp_send.at[c, d], tp_recv.at[c, d],
            device_id={"tp": lax.rem(my_tp + d, n_tp)}, device_id_type=MESH)

    def own(c):
        return pltpu.make_async_copy(relay.at[c, 0], columns(my_tp, c), own_sem.at[c])

    def early_to_tp(d):
        return pltpu.make_async_remote_copy(
            early.at[d - 1], middle.at[d], early_send.at[d], early_recv.at[d],
            device_id={"tp": lax.rem(my_tp + d, n_tp)}, device_id_type=MESH)

    def fan(d):
        return pltpu.make_async_remote_copy(
            middle, spread.at[d - 1], fan_send.at[d], fan_recv.at[d],
            device_id={"ep": lax.rem(my_ep + d, n_ep)}, device_id_type=MESH)

    def late_own(p):
        return pltpu.make_async_copy(late.at[p], columns(lax.rem(my_tp + n_tp - p, n_tp), 0), late_sem.at[p])

    load(0).start()
    span_copy = pltpu.make_async_copy(span_hbm, span, span_sem)
    span_copy.start()

    barrier = pltpu.get_barrier_semaphore()
    for d in range(1, n_ep):
        pl.semaphore_signal(barrier, inc=1, device_id={"ep": lax.rem(my_ep + d, n_ep)}, device_id_type=MESH)
    for d in range(1, n_tp):
        pl.semaphore_signal(barrier, inc=1, device_id={"tp": lax.rem(my_tp + d, n_tp)}, device_id_type=MESH)

    near = my_tp < n_tp // 2
    edge = jnp.where(near, my_tp, n_tp - 1 - my_tp)
    ways = []
    for k in range(n_tp - 1):
        m = k - (n_tp - 1 - 2 * edge)
        half = edge - jnp.maximum(m, 0) // 2
        inner = jnp.where(jnp.maximum(m, 0) % 2 == 0, half, n_tp - half)
        hop = jnp.where(m < 0, n_tp - 1 - edge - k, inner)
        ways.append(jnp.where(near, hop, n_tp - hop))

    span_copy.wait()
    wanted = []
    for d in range(n_ep):
        i = lax.rem(my_ep + d, n_ep)
        total = jnp.int32(0)
        for j in range(n_tp):
            g = span[i, my_dp, j]
            total = total + jnp.where(g // per_expert == my_ep, g % per_expert - my_dp * n_tp, 0)
        wanted.append(total)
    slot = []
    for d in [0] + ways:
        j = lax.rem(my_tp + d, n_tp)
        slot.append(lax.rem(my_ep + n_ep - span[my_ep, my_dp, j] // per_expert, n_ep))

    sooner = []
    for d in [0] + ways:
        j = lax.rem(my_tp + d, n_tp)
        total = jnp.int32(0)
        for i in range(n_ep):
            g = span[i, my_dp, j]
            total = total + jnp.where(g // per_expert == my_ep, g % per_expert - my_dp * n_tp, 0)
        sooner.append(total)

    def turn(c):
        load(c).wait()
        if c == 0:
            for later in range(1, min(STAGES, chunks)):
                load(later).start()

        @pl.loop(0, width // LANES)
        def _(b):
            at = pl.multiple_of(b * LANES, LANES)
            turned[pl.ds(at, LANES), :] = stage[c % STAGES, :, pl.ds(at, LANES)].T

        if c + STAGES < chunks:
            load(c + STAGES).start()

    def block_of(index):
        return pick([turned[b * rows:(b + 1) * rows, :] for b in range(n_tp)], index)

    def first_half(c):
        turn(c)
        for d in range(n_ep - 1, -1, -1):
            if d == 0:
                arrived[c - 1][0] = block_of(wanted[d])
            else:
                send[c, d] = block_of(wanted[d])
                to_ep(c, d).start()

    def second_half(c):
        for d in range(1, n_ep):
            to_ep(c, d).wait_recv()
        for d, index in zip(ways, slot[1:]):
            relay[c, d] = pick([arrived[c - 1][s] for s in range(n_ep)], index)
            to_tp(c, d).start()
        relay[c, 0] = pick([arrived[c - 1][s] for s in range(n_ep)], slot[0])
        own(c).start()

    turn(0)
    for k, d in enumerate(ways):
        early[d - 1] = block_of(sooner[k + 1])
        if k == 0:
            pl.semaphore_wait(barrier, n_ep + n_tp - 2)
        early_to_tp(d).start()
    middle[0] = block_of(sooner[0])

    for step in range(1, chunks + AHEAD):
        if step < chunks:
            first_half(step)
        if step == chunks:
            for d in range(1, n_tp):
                early_to_tp(d).wait_recv()
            for d in range(1, n_ep):
                fan(d).start()
        if step > AHEAD:
            second_half(step - AHEAD)

    for d in range(1, n_ep):
        fan(d).wait_recv()
    for p in range(n_tp):
        late[p] = pick([middle[p]] + [spread[d - 1, p] for d in range(1, n_ep)], slot[0])
        late_own(p).start()

    for d in range(1, n_ep):
        fan(d).wait_send()
    for d in range(1, n_tp):
        early_to_tp(d).wait_send()
    for c in range(1, chunks):
        for d in range(1, n_ep):
            to_ep(c, d).wait_send()
        for d in range(1, n_tp):
            from_tp(c, d).wait_recv()
            to_tp(c, d).wait_send()
        own(c).wait()
    for p in range(n_tp):
        late_own(p).wait()


def writer(saved, out, sem):
    pieces = sem.shape[0]
    rows = saved.shape[2] // pieces
    copies = [
        pltpu.make_async_copy(
            saved.at[0, 0, pl.ds(p * rows, rows)], out.at[0, 0, pl.ds(p * rows, rows)], sem.at[p])
        for p in range(pieces)
    ]
    for copy in copies:
        copy.start()
    for copy in copies:
        copy.wait()


def write_out(saved):
    tiles = max(saved.shape[2] // SUBLANES, 1)
    pieces = max(p for p in range(1, WRITES + 1) if tiles % p == 0)
    return pl.pallas_call(
        writer,
        out_shape=jax.ShapeDtypeStruct(saved.shape, saved.dtype),
        in_specs=[pl.BlockSpec(memory_space=pltpu.VMEM)],
        out_specs=pl.BlockSpec(memory_space=pl.ANY),
        scratch_shapes=[pltpu.SemaphoreType.DMA((pieces,))],
        compiler_params=pltpu.CompilerParams(vmem_limit_bytes=SPARE),
    )(saved)


def local(down_weight, owned_span):
    n_ep, n_tp, n_dp = (lax.axis_size(a) for a in ("ep", "tp", "dp"))
    _, hidden, width = down_weight.shape
    rows = width // n_tp
    chunk = min(CHUNK, hidden)
    chunks = hidden // chunk
    kind = down_weight.dtype
    block = rows * chunk * kind.itemsize
    scratch_bytes = (STAGES + 1) * n_tp * block + chunks * (2 * n_ep + n_tp) * block + (n_ep + 2) * n_tp * block
    saved = pl.pallas_call(
        functools.partial(kernel, n_ep, n_tp, n_dp, chunk),
        out_shape=pltpu.VMEM((1, 1, rows, n_tp * hidden), kind),
        in_specs=[pl.BlockSpec(memory_space=pl.ANY), pl.BlockSpec(memory_space=pl.ANY)],
        out_specs=pl.BlockSpec(memory_space=pltpu.VMEM),
        scratch_shapes=[
            pltpu.VMEM((STAGES, chunk, width), kind),
            pltpu.VMEM((width, chunk), kind),
            pltpu.VMEM((chunks, n_ep, rows, chunk), kind),
            pltpu.VMEM((chunks, n_tp, rows, chunk), kind),
            pltpu.SMEM((n_ep, n_dp, n_tp), jnp.int32),
            pltpu.SemaphoreType.DMA((STAGES,)),
            pltpu.SemaphoreType.DMA,
            pltpu.SemaphoreType.DMA((chunks, n_ep)),
            pltpu.SemaphoreType.DMA((chunks, n_ep)),
            pltpu.SemaphoreType.DMA((chunks, n_tp)),
            pltpu.SemaphoreType.DMA((chunks, n_tp)),
            pltpu.SemaphoreType.DMA((chunks,)),
            pltpu.VMEM((n_tp - 1, rows, chunk), kind),
            pltpu.VMEM((n_tp, rows, chunk), kind),
            pltpu.VMEM((n_ep - 1, n_tp, rows, chunk), kind),
            pltpu.VMEM((n_tp, rows, chunk), kind),
            pltpu.SemaphoreType.DMA((n_tp,)),
            pltpu.SemaphoreType.DMA((n_tp,)),
            pltpu.SemaphoreType.DMA((n_ep,)),
            pltpu.SemaphoreType.DMA((n_ep,)),
            pltpu.SemaphoreType.DMA((n_tp,)),
        ] + [pltpu.VMEM((n_ep, rows, chunk), kind) for _ in range(chunks - 1)],
        compiler_params=pltpu.CompilerParams(
            collective_id=0, has_side_effects=True, vmem_limit_bytes=scratch_bytes + SPARE),
    )(down_weight, jnp.transpose(owned_span, (0, 2, 1)))
    return write_out(saved)


def solution(mesh):
    return jax.shard_map(
        local,
        mesh=mesh,
        in_specs=(P("ep", "tp", "dp"), P()),
        out_specs=P("ep", "tp", "dp", None),
        check_vma=False,
    )
```

```python
import functools

import jax
import jax.numpy as jnp
from jax import lax
from jax.experimental import pallas as pl
from jax.experimental.pallas import tpu as pltpu
from jax.sharding import PartitionSpec as P

MESH = pl.DeviceIdType.MESH
LANES = 128
SUBLANES = 16
CHUNK = 256
STAGES = 4
AHEAD = 2
SPARE = 3 << 20
WRITES = 8
KEEP = (1, 5)


def pick(values, index):
    chosen = values[0]
    for b in range(1, len(values)):
        chosen = jnp.where(index == b, values[b], chosen)
    return chosen


def middle_of(my_tp, n_tp):
    return jnp.logical_or(my_tp == n_tp // 2 - 1, my_tp == n_tp // 2)


def kept_by(my_dp, most):
    return jnp.where(my_dp % 2 == 0, min(KEEP[0], most), min(KEEP[1], most))


def kernel(n_ep, n_tp, n_dp, chunk, most, weight, span_hbm, out, kept, stage, turned, send, relay, span,
           load_sem, span_sem, ep_send, ep_recv, tp_send, tp_recv, own_sem, early, middle, spread, late,
           early_send, early_recv, fan_send, fan_recv, late_sem, *arrived):
    my_ep = lax.axis_index("ep")
    my_tp = lax.axis_index("tp")
    my_dp = lax.axis_index("dp")
    hidden, width = weight.shape[1], weight.shape[2]
    rows = width // n_tp
    chunks = hidden // chunk
    per_expert = n_tp * n_dp
    keep = kept_by(my_dp, most)

    def load(c):
        return pltpu.make_async_copy(
            weight.at[0, pl.ds(c * chunk, chunk)], stage.at[c % STAGES], load_sem.at[c % STAGES])

    def to_ep(c, d):
        return pltpu.make_async_remote_copy(
            send.at[c, d], arrived[c - 1].at[d], ep_send.at[c, d], ep_recv.at[c, d],
            device_id={"ep": lax.rem(my_ep + d, n_ep)}, device_id_type=MESH)

    def columns(tp, c):
        return out.at[0, 0, :, pl.ds(pl.multiple_of(tp * hidden + c * chunk, chunk), chunk)]

    def to_tp(c, d):
        return pltpu.make_async_remote_copy(
            relay.at[c, d], columns(my_tp, c), tp_send.at[c, d], tp_recv.at[c, d],
            device_id={"tp": lax.rem(my_tp + d, n_tp)}, device_id_type=MESH)

    def from_tp(c, d):
        return pltpu.make_async_remote_copy(
            relay.at[c, d], columns(lax.rem(my_tp + n_tp - d, n_tp), c), tp_send.at[c, d], tp_recv.at[c, d],
            device_id={"tp": lax.rem(my_tp + d, n_tp)}, device_id_type=MESH)

    def own(c):
        return pltpu.make_async_copy(relay.at[c, 0], columns(my_tp, c), own_sem.at[c])

    def early_to_tp(d):
        return pltpu.make_async_remote_copy(
            early.at[d - 1], middle.at[d], early_send.at[d], early_recv.at[d],
            device_id={"tp": lax.rem(my_tp + d, n_tp)}, device_id_type=MESH)

    def fan(d):
        return pltpu.make_async_remote_copy(
            middle, spread.at[d - 1], fan_send.at[d], fan_recv.at[d],
            device_id={"ep": lax.rem(my_ep + d, n_ep)}, device_id_type=MESH)

    def late_own(p):
        return pltpu.make_async_copy(late.at[p], columns(lax.rem(my_tp + n_tp - p, n_tp), 0), late_sem.at[p])

    load(0).start()
    span_copy = pltpu.make_async_copy(span_hbm, span, span_sem)
    span_copy.start()

    barrier = pltpu.get_barrier_semaphore()
    for d in range(1, n_ep):
        pl.semaphore_signal(barrier, inc=1, device_id={"ep": lax.rem(my_ep + d, n_ep)}, device_id_type=MESH)
    for d in range(1, n_tp):
        pl.semaphore_signal(barrier, inc=1, device_id={"tp": lax.rem(my_tp + d, n_tp)}, device_id_type=MESH)

    near = my_tp < n_tp // 2
    edge = jnp.where(near, my_tp, n_tp - 1 - my_tp)
    ways = []
    for k in range(n_tp - 1):
        m = k - (n_tp - 1 - 2 * edge)
        half = edge - jnp.maximum(m, 0) // 2
        inner = jnp.where(jnp.maximum(m, 0) % 2 == 0, half, n_tp - half)
        hop = jnp.where(m < 0, n_tp - 1 - edge - k, inner)
        ways.append(jnp.where(near, hop, n_tp - hop))

    span_copy.wait()
    wanted = []
    for d in range(n_ep):
        i = lax.rem(my_ep + d, n_ep)
        total = jnp.int32(0)
        for j in range(n_tp):
            g = span[i, my_dp, j]
            total = total + jnp.where(g // per_expert == my_ep, g % per_expert - my_dp * n_tp, 0)
        wanted.append(total)
    slot = []
    for d in [0] + ways:
        j = lax.rem(my_tp + d, n_tp)
        slot.append(lax.rem(my_ep + n_ep - span[my_ep, my_dp, j] // per_expert, n_ep))

    sooner = []
    for d in [0] + ways:
        j = lax.rem(my_tp + d, n_tp)
        total = jnp.int32(0)
        for i in range(n_ep):
            g = span[i, my_dp, j]
            total = total + jnp.where(g // per_expert == my_ep, g % per_expert - my_dp * n_tp, 0)
        sooner.append(total)

    def turn(c):
        load(c).wait()
        if c == 0:
            for later in range(1, min(STAGES, chunks)):
                load(later).start()

        @pl.loop(0, width // LANES)
        def _(b):
            at = pl.multiple_of(b * LANES, LANES)
            turned[pl.ds(at, LANES), :] = stage[c % STAGES, :, pl.ds(at, LANES)].T

        if c + STAGES < chunks:
            load(c + STAGES).start()

    def block_of(index):
        return pick([turned[b * rows:(b + 1) * rows, :] for b in range(n_tp)], index)

    def first_half(c):
        turn(c)
        for d in range(n_ep - 1, -1, -1):
            if d == 0:
                arrived[c - 1][0] = block_of(wanted[d])
            else:
                send[c, d] = block_of(wanted[d])
                to_ep(c, d).start()

    def second_half(c):
        for d in range(1, n_ep):
            to_ep(c, d).wait_recv()
        for k, (d, index) in enumerate(zip(ways, slot[1:])):
            piece = pick([arrived[c - 1][s] for s in range(n_ep)], index)
            relay[c, d] = piece
            p = chunks - 1 - c
            if k == n_tp - 3 and p < most:
                kept[p] = piece
                stays = jnp.logical_and(edge == n_tp // 2 - 1, p < keep)
                pl.when(jnp.logical_not(stays))(to_tp(c, d).start)
            else:
                to_tp(c, d).start()
        relay[c, 0] = pick([arrived[c - 1][s] for s in range(n_ep)], slot[0])
        own(c).start()

    turn(0)
    for k, d in enumerate(ways):
        early[d - 1] = block_of(sooner[k + 1])
        if k == 0:
            pl.semaphore_wait(barrier, n_ep + n_tp - 2)
        early_to_tp(d).start()
    middle[0] = block_of(sooner[0])

    for step in range(1, chunks + AHEAD):
        if step < chunks:
            first_half(step)
        if step == chunks:
            for d in range(1, n_tp):
                early_to_tp(d).wait_recv()
            for d in range(1, n_ep):
                fan(d).start()
        if step > AHEAD:
            second_half(step - AHEAD)

    for d in range(1, n_ep):
        fan(d).wait_recv()
    for p in range(n_tp):
        late[p] = pick([middle[p]] + [spread[d - 1, p] for d in range(1, n_ep)], slot[0])
        late_own(p).start()

    for d in range(1, n_ep):
        fan(d).wait_send()
    for d in range(1, n_tp):
        early_to_tp(d).wait_send()
    for c in range(1, chunks):
        for d in range(1, n_ep):
            to_ep(c, d).wait_send()
        for d in range(1, n_tp):
            p = chunks - 1 - c
            if p < most and d in (1, n_tp - 1):
                low, high = my_tp == n_tp // 2 - 1, my_tp == n_tp // 2
                sent, got = (low, high) if d == 1 else (high, low)
                pl.when(jnp.logical_not(jnp.logical_and(got, p < keep)))(from_tp(c, d).wait_recv)
                pl.when(jnp.logical_not(jnp.logical_and(sent, p < keep)))(to_tp(c, d).wait_send)
            else:
                from_tp(c, d).wait_recv()
                to_tp(c, d).wait_send()
        own(c).wait()
    for p in range(n_tp):
        late_own(p).wait()


def writer(saved, out, token, sem):
    pieces = sem.shape[0]
    rows = saved.shape[2] // pieces
    copies = [
        pltpu.make_async_copy(
            saved.at[0, 0, pl.ds(p * rows, rows)], out.at[0, 0, pl.ds(p * rows, rows)], sem.at[p])
        for p in range(pieces)
    ]
    for copy in copies:
        copy.start()
    for copy in copies:
        copy.wait()
    token[...] = jnp.zeros_like(token)


def write_out(saved):
    tiles = max(saved.shape[2] // SUBLANES, 1)
    pieces = max(p for p in range(1, WRITES + 1) if tiles % p == 0)
    return pl.pallas_call(
        writer,
        out_shape=(jax.ShapeDtypeStruct(saved.shape, saved.dtype), pltpu.VMEM((8, LANES), jnp.float32)),
        in_specs=[pl.BlockSpec(memory_space=pltpu.VMEM)],
        out_specs=(pl.BlockSpec(memory_space=pl.ANY), pl.BlockSpec(memory_space=pltpu.VMEM)),
        scratch_shapes=[pltpu.SemaphoreType.DMA((pieces,))],
        compiler_params=pltpu.CompilerParams(vmem_limit_bytes=SPARE),
    )(saved)


def swap(n_tp, kept, token, got, send_sem, recv_sem):
    my_tp = lax.axis_index("tp")
    other = n_tp - 1 - my_tp
    most = kept.shape[0]
    keep = kept_by(lax.axis_index("dp"), most)

    @pl.when(middle_of(my_tp, n_tp))
    def _():
        barrier = pltpu.get_barrier_semaphore()
        pl.semaphore_signal(barrier, inc=1, device_id={"tp": other}, device_id_type=MESH)
        pl.semaphore_wait(barrier, 1)
        copies = [
            pltpu.make_async_remote_copy(
                kept.at[p], got.at[p], send_sem.at[p], recv_sem.at[p],
                device_id={"tp": other}, device_id_type=MESH)
            for p in range(most)
        ]
        for p in reversed(range(most)):
            pl.when(p < keep)(copies[p].start)
        for p in reversed(range(most)):
            pl.when(p < keep)(copies[p].wait)


def exchange(n_tp, kept, token):
    return pl.pallas_call(
        functools.partial(swap, n_tp),
        out_shape=pltpu.VMEM(kept.shape, kept.dtype),
        in_specs=[pl.BlockSpec(memory_space=pltpu.VMEM)] * 2,
        out_specs=pl.BlockSpec(memory_space=pltpu.VMEM),
        scratch_shapes=[pltpu.SemaphoreType.DMA((kept.shape[0],)), pltpu.SemaphoreType.DMA((kept.shape[0],))],
        compiler_params=pltpu.CompilerParams(collective_id=1, has_side_effects=True, vmem_limit_bytes=SPARE),
    )(kept, token)


def finish(n_tp, hidden, got, written, out, sem):
    del written
    my_tp = lax.axis_index("tp")
    most, _, chunk = got.shape
    keep = kept_by(lax.axis_index("dp"), most)

    @pl.when(middle_of(my_tp, n_tp))
    def _():
        end = (n_tp - my_tp) * hidden
        copies = [
            pltpu.make_async_copy(
                got.at[p], out.at[0, 0, :, pl.ds(pl.multiple_of(end - (p + 1) * chunk, chunk), chunk)], sem.at[p])
            for p in range(most)
        ]
        for p in range(most):
            pl.when(p < keep)(copies[p].start)
        for p in range(most):
            pl.when(p < keep)(copies[p].wait)


def write_rest(n_tp, hidden, got, written):
    return pl.pallas_call(
        functools.partial(finish, n_tp, hidden),
        out_shape=jax.ShapeDtypeStruct(written.shape, written.dtype),
        in_specs=[pl.BlockSpec(memory_space=pltpu.VMEM), pl.BlockSpec(memory_space=pl.ANY)],
        out_specs=pl.BlockSpec(memory_space=pl.ANY),
        scratch_shapes=[pltpu.SemaphoreType.DMA((got.shape[0],))],
        input_output_aliases={1: 0},
        compiler_params=pltpu.CompilerParams(vmem_limit_bytes=SPARE),
    )(got, written)


def local(down_weight, owned_span):
    n_ep, n_tp, n_dp = (lax.axis_size(a) for a in ("ep", "tp", "dp"))
    _, hidden, width = down_weight.shape
    rows = width // n_tp
    chunk = min(CHUNK, hidden)
    chunks = hidden // chunk
    most = min(max(KEEP), chunks - 1)
    kind = down_weight.dtype
    block = rows * chunk * kind.itemsize
    scratch_bytes = (STAGES + 1) * n_tp * block + chunks * (2 * n_ep + n_tp) * block + (n_ep + 2) * n_tp * block
    saved, kept = pl.pallas_call(
        functools.partial(kernel, n_ep, n_tp, n_dp, chunk, most),
        out_shape=(pltpu.VMEM((1, 1, rows, n_tp * hidden), kind), pltpu.VMEM((most, rows, chunk), kind)),
        in_specs=[pl.BlockSpec(memory_space=pl.ANY), pl.BlockSpec(memory_space=pl.ANY)],
        out_specs=(pl.BlockSpec(memory_space=pltpu.VMEM), pl.BlockSpec(memory_space=pltpu.VMEM)),
        scratch_shapes=[
            pltpu.VMEM((STAGES, chunk, width), kind),
            pltpu.VMEM((width, chunk), kind),
            pltpu.VMEM((chunks, n_ep, rows, chunk), kind),
            pltpu.VMEM((chunks, n_tp, rows, chunk), kind),
            pltpu.SMEM((n_ep, n_dp, n_tp), jnp.int32),
            pltpu.SemaphoreType.DMA((STAGES,)),
            pltpu.SemaphoreType.DMA,
            pltpu.SemaphoreType.DMA((chunks, n_ep)),
            pltpu.SemaphoreType.DMA((chunks, n_ep)),
            pltpu.SemaphoreType.DMA((chunks, n_tp)),
            pltpu.SemaphoreType.DMA((chunks, n_tp)),
            pltpu.SemaphoreType.DMA((chunks,)),
            pltpu.VMEM((n_tp - 1, rows, chunk), kind),
            pltpu.VMEM((n_tp, rows, chunk), kind),
            pltpu.VMEM((n_ep - 1, n_tp, rows, chunk), kind),
            pltpu.VMEM((n_tp, rows, chunk), kind),
            pltpu.SemaphoreType.DMA((n_tp,)),
            pltpu.SemaphoreType.DMA((n_tp,)),
            pltpu.SemaphoreType.DMA((n_ep,)),
            pltpu.SemaphoreType.DMA((n_ep,)),
            pltpu.SemaphoreType.DMA((n_tp,)),
        ] + [pltpu.VMEM((n_ep, rows, chunk), kind) for _ in range(chunks - 1)],
        compiler_params=pltpu.CompilerParams(
            collective_id=0, has_side_effects=True, vmem_limit_bytes=scratch_bytes + SPARE),
    )(down_weight, jnp.transpose(owned_span, (0, 2, 1)))
    written, token = write_out(saved)
    return write_rest(n_tp, hidden, exchange(n_tp, kept, token), written)


def solution(mesh):
    return jax.shard_map(
        local,
        mesh=mesh,
        in_specs=(P("ep", "tp", "dp"), P()),
        out_specs=P("ep", "tp", "dp", None),
        check_vma=False,
    )
```

```python
import functools

import jax
import jax.numpy as jnp
from jax import lax
from jax.experimental import pallas as pl
from jax.experimental.pallas import tpu as pltpu
from jax.sharding import PartitionSpec as P

MESH = pl.DeviceIdType.MESH
LANES = 128
SUBLANES = 16
CHUNK = 256
STAGES = 4
AHEAD = 2
SPARE = 3 << 20
VMEM_BYTES = 67043328
WRITES = 8
KEEP = (2, 5)


def pick(values, index):
    chosen = values[0]
    for b in range(1, len(values)):
        chosen = jnp.where(index == b, values[b], chosen)
    return chosen


def middle_of(my_tp, n_tp):
    return jnp.logical_or(my_tp == n_tp // 2 - 1, my_tp == n_tp // 2)


def kept_by(my_dp, most):
    return jnp.where(my_dp % 2 == 0, min(KEEP[0], most), min(KEEP[1], most))


def kept_counts(most):
    return sorted({min(k, most) for k in KEEP})


def kernel(n_ep, n_tp, n_dp, chunk, most, weight, span_hbm, out, kept, stage, turned, send, relay, span,
           early, middle, spread, load_sem, span_sem, ep_send, ep_recv, tp_send, tp_recv, late_send, late_recv,
           early_send, early_recv, fan_send, fan_recv, *arrived):
    my_ep = lax.axis_index("ep")
    my_tp = lax.axis_index("tp")
    my_dp = lax.axis_index("dp")
    hidden, width = weight.shape[1], weight.shape[2]
    rows = width // n_tp
    chunks = hidden // chunk
    per_expert = n_tp * n_dp
    keep = kept_by(my_dp, most)
    mid = middle_of(my_tp, n_tp)
    others = jnp.logical_not(mid)

    near = my_tp < n_tp // 2
    edge = jnp.where(near, my_tp, n_tp - 1 - my_tp)
    ways = []
    for k in range(n_tp - 1):
        m = k - (n_tp - 1 - 2 * edge)
        half = edge - jnp.maximum(m, 0) // 2
        inner = jnp.where(jnp.maximum(m, 0) % 2 == 0, half, n_tp - half)
        hop = jnp.where(m < 0, n_tp - 1 - edge - k, inner)
        ways.append(jnp.where(near, hop, n_tp - hop))
    across = n_tp - 3

    def load(c):
        return pltpu.make_async_copy(
            weight.at[0, pl.ds(c * chunk, chunk)], stage.at[c % STAGES], load_sem.at[c % STAGES])

    def remote(src, dst, send_sem, recv_sem, axis, d, n):
        me = my_ep if axis == "ep" else my_tp
        return pltpu.make_async_remote_copy(
            src, dst, send_sem, recv_sem, device_id={axis: lax.rem(me + d, n)}, device_id_type=MESH)

    def to_ep(c, d):
        return remote(send.at[(c - 1) * (n_ep - 1) + d - 1], arrived[c - 1].at[d], ep_send, ep_recv.at[c - 1], "ep", d, n_ep)

    def columns(tp, c):
        return pl.ds(pl.multiple_of(tp * hidden + c * chunk, chunk), chunk)

    def to_tp(c, k, send_sem, recv_sem):
        return remote(
            relay.at[(c - 1) * (n_tp - 1) + k], out.at[0, 0, :, columns(my_tp, c)], send_sem, recv_sem, "tp", ways[k], n_tp)

    def early_to_tp(k):
        return remote(early.at[k], middle.at[ways[k]], early_send, early_recv, "tp", ways[k], n_tp)

    def fan(d):
        return remote(middle, spread.at[d - 1], fan_send, fan_recv, "ep", d, n_ep)

    def ep_sent():
        return remote(send, send, ep_send, ep_recv.at[0], "ep", 1, n_ep)

    def ep_got(c):
        here = arrived[c - 1].at[pl.ds(1, n_ep - 1)]
        return remote(here, here, ep_send, ep_recv.at[c - 1], "ep", 1, n_ep)

    def all_tp(blocks):
        return remote(
            relay.at[pl.ds(0, blocks)], out.at[0, 0, :, pl.ds(0, blocks * chunk)], tp_send, tp_recv, "tp", 1, n_tp)

    def all_early():
        return remote(early, middle.at[pl.ds(1, n_tp - 1)], early_send, early_recv, "tp", 1, n_tp)

    def all_fan():
        return remote(spread, spread, fan_send, fan_recv, "ep", 1, n_ep)

    load(0).start()
    barrier = pltpu.get_barrier_semaphore()
    for d in range(1, n_tp):
        pl.semaphore_signal(barrier, inc=1, device_id={"tp": lax.rem(my_tp + d, n_tp)}, device_id_type=MESH)
    for d in range(n_ep - 1, 0, -1):
        pl.semaphore_signal(barrier, inc=1, device_id={"ep": lax.rem(my_ep + d, n_ep)}, device_id_type=MESH)
    span_copy = pltpu.make_async_copy(span_hbm, span, span_sem)
    span_copy.start()
    span_copy.wait()

    wanted = []
    for d in range(n_ep):
        i = lax.rem(my_ep + d, n_ep)
        total = jnp.int32(0)
        for j in range(n_tp):
            g = span[i, my_dp, j]
            total = total + jnp.where(g // per_expert == my_ep, g % per_expert - my_dp * n_tp, 0)
        wanted.append(total)
    slot = []
    for d in [0] + ways:
        j = lax.rem(my_tp + d, n_tp)
        slot.append(lax.rem(my_ep + n_ep - span[my_ep, my_dp, j] // per_expert, n_ep))

    sooner = []
    for d in [0] + ways:
        j = lax.rem(my_tp + d, n_tp)
        total = jnp.int32(0)
        for i in range(n_ep):
            g = span[i, my_dp, j]
            total = total + jnp.where(g // per_expert == my_ep, g % per_expert - my_dp * n_tp, 0)
        sooner.append(total)

    def turn(c):
        load(c).wait()

        @pl.loop(0, width // LANES)
        def _(b):
            at = pl.multiple_of(b * LANES, LANES)
            turned[pl.ds(at, LANES), :] = stage[c % STAGES, :, pl.ds(at, LANES)].T

        if c + STAGES < chunks:
            load(c + STAGES).start()

    def block_of(index):
        return pick([turned[b * rows:(b + 1) * rows, :] for b in range(n_tp)], index)

    def first_block(target, index):
        if rows % LANES:
            target[...] = block_of(index)
            return
        for q in range(0, rows, LANES):
            tiles = [stage[0, :, b * rows + q:b * rows + q + LANES] for b in range(n_tp)]
            target[q:q + LANES, :] = pick(tiles, index).T

    def first_half(c):
        turn(c)
        for d in range(n_ep - 1, -1, -1):
            if d == 0:
                arrived[c - 1][0] = block_of(wanted[d])
            else:
                send[(c - 1) * (n_ep - 1) + d - 1] = block_of(wanted[d])
                to_ep(c, d).start()

    def second_half(c):
        ep_got(c).wait_recv()
        p = chunks - 1 - c
        for k in range(n_tp - 1):
            piece = pick([arrived[c - 1][s] for s in range(n_ep)], slot[k + 1])
            relay[(c - 1) * (n_tp - 1) + k] = piece
            if k == across and p < most:
                kept[:, (most - 1 - p) * chunk:(most - p) * chunk] = piece
                pl.when(others)(to_tp(c, k, tp_send, tp_recv).start)
                pl.when(jnp.logical_and(mid, p >= keep))(to_tp(c, k, late_send.at[p], late_recv.at[p]).start)
            else:
                to_tp(c, k, tp_send, tp_recv).start()
        out[0, 0, :, columns(my_tp, c)] = pick([arrived[c - 1][s] for s in range(n_ep)], slot[0])

    if rows % LANES:
        turn(0)
    else:
        load(0).wait()
    for later in range(1, min(STAGES, chunks)):
        load(later).start()
    for k in range(n_tp - 1):
        first_block(early.at[k], sooner[k + 1])
        if k == 0:
            pl.semaphore_wait(barrier, n_ep + n_tp - 2)
        early_to_tp(k).start()
    first_block(middle.at[0], sooner[0])
    if rows % LANES == 0 and STAGES < chunks:
        load(STAGES).start()

    for step in range(1, chunks + AHEAD):
        if step < chunks:
            first_half(step)
        if step == chunks:
            all_early().wait_recv()
            for d in range(1, n_ep):
                fan(d).start()
        if step > AHEAD:
            second_half(step - AHEAD)

    all_fan().wait_recv()
    for p in range(n_tp):
        found = pick([middle[p]] + [spread[d - 1, p] for d in range(1, n_ep)], slot[0])
        out[0, 0, :, columns(lax.rem(my_tp + n_tp - p, n_tp), 0)] = found

    all_fan().wait_send()
    all_early().wait_send()
    ep_sent().wait_send()
    blocks = (chunks - 1) * (n_tp - 1)

    @pl.when(others)
    def _():
        all_tp(blocks).wait()

    @pl.when(mid)
    def _():
        all_tp(blocks - most).wait()

    for p in range(most):
        pl.when(jnp.logical_and(mid, p >= keep))(
            to_tp(chunks - 1 - p, across, late_send.at[p], late_recv.at[p]).wait)


def writer(saved, out, token, sem):
    pieces = sem.shape[0]
    rows = saved.shape[2] // pieces
    copies = [
        pltpu.make_async_copy(
            saved.at[0, 0, pl.ds(p * rows, rows)], out.at[0, 0, pl.ds(p * rows, rows)], sem.at[p])
        for p in range(pieces)
    ]
    for copy in copies:
        copy.start()
    for copy in copies:
        copy.wait()
    token[...] = jnp.zeros_like(token)


def write_out(saved):
    tiles = max(saved.shape[2] // SUBLANES, 1)
    pieces = max(p for p in range(1, WRITES + 1) if tiles % p == 0)
    return pl.pallas_call(
        writer,
        out_shape=(jax.ShapeDtypeStruct(saved.shape, saved.dtype), pltpu.VMEM((8, LANES), jnp.float32)),
        in_specs=[pl.BlockSpec(memory_space=pltpu.VMEM)],
        out_specs=(pl.BlockSpec(memory_space=pl.ANY), pl.BlockSpec(memory_space=pltpu.VMEM)),
        scratch_shapes=[pltpu.SemaphoreType.DMA((pieces,))],
        compiler_params=pltpu.CompilerParams(vmem_limit_bytes=SPARE),
    )(saved)


def swap(n_tp, chunk, kept, token, got, send_sem, recv_sem):
    del token
    my_tp = lax.axis_index("tp")
    other = n_tp - 1 - my_tp
    most = kept.shape[1] // chunk
    keep = kept_by(lax.axis_index("dp"), most)

    @pl.when(middle_of(my_tp, n_tp))
    def _():
        barrier = pltpu.get_barrier_semaphore()
        pl.semaphore_signal(barrier, inc=1, device_id={"tp": other}, device_id_type=MESH)
        pl.semaphore_wait(barrier, 1)
        for count in kept_counts(most):
            part = pl.ds((most - count) * chunk, count * chunk)
            copy = pltpu.make_async_remote_copy(
                kept.at[:, part], got.at[:, part], send_sem, recv_sem,
                device_id={"tp": other}, device_id_type=MESH)
            pl.when(keep == count)(copy.start)
        for count in kept_counts(most):
            part = pl.ds((most - count) * chunk, count * chunk)
            copy = pltpu.make_async_remote_copy(
                kept.at[:, part], got.at[:, part], send_sem, recv_sem,
                device_id={"tp": other}, device_id_type=MESH)
            pl.when(keep == count)(copy.wait)


def exchange(n_tp, chunk, kept, token):
    return pl.pallas_call(
        functools.partial(swap, n_tp, chunk),
        out_shape=pltpu.VMEM(kept.shape, kept.dtype),
        in_specs=[pl.BlockSpec(memory_space=pltpu.VMEM)] * 2,
        out_specs=pl.BlockSpec(memory_space=pltpu.VMEM),
        scratch_shapes=[pltpu.SemaphoreType.DMA, pltpu.SemaphoreType.DMA],
        compiler_params=pltpu.CompilerParams(collective_id=1, has_side_effects=True, vmem_limit_bytes=SPARE),
    )(kept, token)


def finish(n_tp, hidden, chunk, got, written, out, sem):
    del written
    my_tp = lax.axis_index("tp")
    most = got.shape[1] // chunk
    keep = kept_by(lax.axis_index("dp"), most)
    end = (n_tp - my_tp) * hidden

    @pl.when(middle_of(my_tp, n_tp))
    def _():
        for count in kept_counts(most):
            size = count * chunk
            copy = pltpu.make_async_copy(
                got.at[:, pl.ds((most - count) * chunk, size)],
                out.at[0, 0, :, pl.ds(pl.multiple_of(end - size, chunk), size)], sem)

            @pl.when(keep == count)
            def _():
                copy.start()
                copy.wait()


def write_rest(n_tp, hidden, chunk, got, written):
    return pl.pallas_call(
        functools.partial(finish, n_tp, hidden, chunk),
        out_shape=jax.ShapeDtypeStruct(written.shape, written.dtype),
        in_specs=[pl.BlockSpec(memory_space=pltpu.VMEM), pl.BlockSpec(memory_space=pl.ANY)],
        out_specs=pl.BlockSpec(memory_space=pl.ANY),
        scratch_shapes=[pltpu.SemaphoreType.DMA],
        input_output_aliases={1: 0},
        compiler_params=pltpu.CompilerParams(vmem_limit_bytes=SPARE),
    )(got, written)


def local(down_weight, owned_span):
    n_ep, n_tp, n_dp = (lax.axis_size(a) for a in ("ep", "tp", "dp"))
    _, hidden, width = down_weight.shape
    rows = width // n_tp
    chunk = min(CHUNK, hidden)
    chunks = hidden // chunk
    most = min(max(KEEP), chunks - 1)
    kind = down_weight.dtype
    results = (n_tp * hidden + most * chunk) * rows * kind.itemsize
    saved, kept = pl.pallas_call(
        functools.partial(kernel, n_ep, n_tp, n_dp, chunk, most),
        out_shape=(pltpu.VMEM((1, 1, rows, n_tp * hidden), kind), pltpu.VMEM((rows, most * chunk), kind)),
        in_specs=[pl.BlockSpec(memory_space=pl.ANY), pl.BlockSpec(memory_space=pl.ANY)],
        out_specs=(pl.BlockSpec(memory_space=pltpu.VMEM), pl.BlockSpec(memory_space=pltpu.VMEM)),
        scratch_shapes=[
            pltpu.VMEM((STAGES, chunk, width), kind),
            pltpu.VMEM((width, chunk), kind),
            pltpu.VMEM(((chunks - 1) * (n_ep - 1), rows, chunk), kind),
            pltpu.VMEM(((chunks - 1) * (n_tp - 1), rows, chunk), kind),
            pltpu.SMEM((n_ep, n_dp, n_tp), jnp.int32),
            pltpu.VMEM((n_tp - 1, rows, chunk), kind),
            pltpu.VMEM((n_tp, rows, chunk), kind),
            pltpu.VMEM((n_ep - 1, n_tp, rows, chunk), kind),
            pltpu.SemaphoreType.DMA((STAGES,)),
            pltpu.SemaphoreType.DMA,
            pltpu.SemaphoreType.DMA,
            pltpu.SemaphoreType.DMA((chunks - 1,)),
            pltpu.SemaphoreType.DMA,
            pltpu.SemaphoreType.DMA,
            pltpu.SemaphoreType.DMA((most,)),
            pltpu.SemaphoreType.DMA((most,)),
            pltpu.SemaphoreType.DMA,
            pltpu.SemaphoreType.DMA,
            pltpu.SemaphoreType.DMA,
            pltpu.SemaphoreType.DMA,
        ] + [pltpu.VMEM((n_ep, rows, chunk), kind) for _ in range(chunks - 1)],
        compiler_params=pltpu.CompilerParams(
            collective_id=0, has_side_effects=True, vmem_limit_bytes=VMEM_BYTES - results),
    )(down_weight, jnp.transpose(owned_span, (0, 2, 1)))
    written, token = write_out(saved)
    return write_rest(n_tp, hidden, chunk, exchange(n_tp, chunk, kept, token), written)


def solution(mesh):
    return jax.shard_map(
        local,
        mesh=mesh,
        in_specs=(P("ep", "tp", "dp"), P()),
        out_specs=P("ep", "tp", "dp", None),
        check_vma=False,
    )
```

```python
import functools

import jax
import jax.numpy as jnp
from jax import lax
from jax.experimental import pallas as pl
from jax.experimental.pallas import tpu as pltpu
from jax.sharding import PartitionSpec as P

MESH = pl.DeviceIdType.MESH
LANES = 128
SUBLANES = 16
CHUNK = 256
STAGES = 4
AHEAD = 2
SPARE = 3 << 20
VMEM_BYTES = 67043328
WRITES = 8
KEEP = (2, 5)


def pick(values, index):
    chosen = values[0]
    for b in range(1, len(values)):
        chosen = jnp.where(index == b, values[b], chosen)
    return chosen


def middle_of(my_tp, n_tp):
    return jnp.logical_or(my_tp == n_tp // 2 - 1, my_tp == n_tp // 2)


def kept_by(my_dp, most):
    return jnp.where(my_dp % 2 == 0, min(KEEP[0], most), min(KEEP[1], most))


def kept_counts(most):
    return sorted({min(k, most) for k in KEEP})


def kernel(n_ep, n_tp, n_dp, chunk, most, weight, span_hbm, out, kept, stage, turned, send, relay, span,
           early, middle, spread, load_sem, span_sem, ep_send, ep_recv, tp_send, tp_recv, late_send, late_recv,
           early_send, early_recv, fan_send, fan_recv, settled, ready, *arrived):
    my_ep = lax.axis_index("ep")
    my_tp = lax.axis_index("tp")
    my_dp = lax.axis_index("dp")
    hidden, width = weight.shape[1], weight.shape[2]
    rows = width // n_tp
    chunks = hidden // chunk
    per_expert = n_tp * n_dp
    keep = kept_by(my_dp, most)
    mid = middle_of(my_tp, n_tp)
    others = jnp.logical_not(mid)

    near = my_tp < n_tp // 2
    edge = jnp.where(near, my_tp, n_tp - 1 - my_tp)
    ways = []
    for k in range(n_tp - 1):
        m = k - (n_tp - 1 - 2 * edge)
        half = edge - jnp.maximum(m, 0) // 2
        inner = jnp.where(jnp.maximum(m, 0) % 2 == 0, half, n_tp - half)
        hop = jnp.where(m < 0, n_tp - 1 - edge - k, inner)
        ways.append(jnp.where(near, hop, n_tp - hop))
    across = n_tp - 3

    def load(c):
        return pltpu.make_async_copy(
            weight.at[0, pl.ds(c * chunk, chunk)], stage.at[c % STAGES], load_sem.at[c % STAGES])

    def remote(src, dst, send_sem, recv_sem, axis, d, n):
        me = my_ep if axis == "ep" else my_tp
        return pltpu.make_async_remote_copy(
            src, dst, send_sem, recv_sem, device_id={axis: lax.rem(me + d, n)}, device_id_type=MESH)

    def to_ep(c, d):
        return remote(send.at[(c - 1) * (n_ep - 1) + d - 1], arrived[c - 1].at[d], ep_send, ep_recv.at[c - 1], "ep", d, n_ep)

    def columns(tp, c):
        return pl.ds(pl.multiple_of(tp * hidden + c * chunk, chunk), chunk)

    def to_tp(c, k, send_sem, recv_sem):
        return remote(
            relay.at[(c - 1) * (n_tp - 1) + k], out.at[0, 0, :, columns(my_tp, c)], send_sem, recv_sem, "tp", ways[k], n_tp)

    def early_to_tp(k):
        return remote(early.at[k], middle.at[ways[k]], early_send, early_recv, "tp", ways[k], n_tp)

    def fan(d):
        return remote(middle, spread.at[d - 1], fan_send, fan_recv, "ep", d, n_ep)

    def ep_sent():
        return remote(send, send, ep_send, ep_recv.at[0], "ep", 1, n_ep)

    def ep_got(c):
        here = arrived[c - 1].at[pl.ds(1, n_ep - 1)]
        return remote(here, here, ep_send, ep_recv.at[c - 1], "ep", 1, n_ep)

    def all_tp(blocks):
        return remote(
            relay.at[pl.ds(0, blocks)], out.at[0, 0, :, pl.ds(0, blocks * chunk)], tp_send, tp_recv, "tp", 1, n_tp)

    def all_early():
        return remote(early, middle.at[pl.ds(1, n_tp - 1)], early_send, early_recv, "tp", 1, n_tp)

    def all_fan():
        return remote(spread, spread, fan_send, fan_recv, "ep", 1, n_ep)

    load(0).start()
    barrier = pltpu.get_barrier_semaphore()

    def tell(sem, axis, index):
        pl.semaphore_signal(sem, inc=1, device_id={axis: index}, device_id_type=MESH)

    ep_peers = [lax.rem(my_ep + d, n_ep) for d in range(n_ep - 1, 0, -1)]
    tp_peers = [lax.rem(my_tp + d, n_tp) for d in range(1, n_tp)]

    @pl.when(mid)
    def _():
        tell(barrier, "tp", n_tp - 1 - my_tp)

    @pl.when(others)
    def _():
        for peer in tp_peers:
            pl.when(jnp.logical_not(middle_of(peer, n_tp)))(functools.partial(tell, barrier, "tp", peer))
        for peer in ep_peers:
            tell(barrier, "ep", peer)

    span_copy = pltpu.make_async_copy(span_hbm, span, span_sem)
    span_copy.start()
    span_copy.wait()

    def block_here(g):
        return jnp.where(lax.div(g, per_expert) == my_ep, lax.rem(g, per_expert) - my_dp * n_tp, 0)

    def sooner(d):
        j = lax.rem(my_tp + d, n_tp)
        return sum((block_here(span[i, my_dp, j]) for i in range(n_ep)), jnp.int32(0))

    def turn(c):
        load(c).wait()

        @pl.loop(0, width // LANES)
        def _(b):
            at = pl.multiple_of(b * LANES, LANES)
            turned[pl.ds(at, LANES), :] = stage[c % STAGES, :, pl.ds(at, LANES)].T

        if c + STAGES < chunks:
            load(c + STAGES).start()

    def block_of(index):
        return pick([turned[b * rows:(b + 1) * rows, :] for b in range(n_tp)], index)

    def first_block(target, index):
        if rows % LANES:
            target[...] = block_of(index)
            return
        for q in range(0, rows, LANES):
            tiles = [stage[0, :, b * rows + q:b * rows + q + LANES] for b in range(n_tp)]
            target[q:q + LANES, :] = pick(tiles, index).T

    def first_half(c):
        if c > 1:
            turn(c)
        for d in range(n_ep - 1, -1, -1):
            if d == 0:
                arrived[c - 1][0] = block_of(wanted[d])
            else:
                send[(c - 1) * (n_ep - 1) + d - 1] = block_of(wanted[d])
                to_ep(c, d).start()

    def second_half(c):
        ep_got(c).wait_recv()
        p = chunks - 1 - c
        for k in range(n_tp - 1):
            piece = pick([arrived[c - 1][s] for s in range(n_ep)], slot[k + 1])
            relay[(c - 1) * (n_tp - 1) + k] = piece
            if k == across and p < most:
                kept[:, (most - 1 - p) * chunk:(most - p) * chunk] = piece
                pl.when(others)(to_tp(c, k, tp_send, tp_recv).start)
                pl.when(jnp.logical_and(mid, p >= keep))(to_tp(c, k, late_send.at[p], late_recv.at[p]).start)
            else:
                to_tp(c, k, tp_send, tp_recv).start()
        out[0, 0, :, columns(my_tp, c)] = pick([arrived[c - 1][s] for s in range(n_ep)], slot[0])

    if rows % LANES:
        turn(0)
    else:
        load(0).wait()
    def start_loads():
        for later in range(1, min(STAGES, chunks)):
            load(later).start()

    later_places = [k for k in range(n_tp - 1) if k != across]

    @pl.when(mid)
    def _():
        first_block(early.at[across], sooner(ways[across]))
        pl.semaphore_wait(barrier, 1)
        early_to_tp(across).start()
        start_loads()
        for peer in tp_peers:
            pl.when(jnp.logical_not(middle_of(peer, n_tp)))(functools.partial(tell, barrier, "tp", peer))
        for k in later_places:
            first_block(early.at[k], sooner(ways[k]))
        first_block(middle.at[0], sooner(0))

    @pl.when(others)
    def _():
        start_loads()
        for k in range(n_tp - 1):
            first_block(early.at[k], sooner(ways[k]))
        first_block(middle.at[0], sooner(0))
        pl.semaphore_wait(barrier, n_ep + n_tp - 2)
        for peer in ep_peers:
            tell(settled, "ep", peer)
        for k in range(n_tp - 1):
            early_to_tp(k).start()

    if rows % LANES == 0 and STAGES < chunks:
        load(STAGES).start()
    turn(1)

    wanted = []
    for d in range(n_ep):
        i = lax.rem(my_ep + d, n_ep)
        wanted.append(sum((block_here(span[i, my_dp, j]) for j in range(n_tp)), jnp.int32(0)))
    slot = []
    for d in [0] + ways:
        j = lax.rem(my_tp + d, n_tp)
        slot.append(lax.rem(my_ep + n_ep - lax.div(span[my_ep, my_dp, j], per_expert), n_ep))

    @pl.when(others)
    def _():
        pl.semaphore_wait(settled, n_ep - 1)
        for peer in tp_peers:
            pl.when(middle_of(peer, n_tp))(functools.partial(tell, ready, "tp", peer))

    @pl.when(mid)
    def _():
        pl.semaphore_wait(ready, n_tp - 2)
        for k in later_places:
            early_to_tp(k).start()

    for step in range(1, chunks + AHEAD):
        if step < chunks:
            first_half(step)
        if step == chunks:
            all_early().wait_recv()
            for d in range(1, n_ep):
                fan(d).start()
        if step > AHEAD:
            second_half(step - AHEAD)

    all_fan().wait_recv()
    for p in range(n_tp):
        found = pick([middle[p]] + [spread[d - 1, p] for d in range(1, n_ep)], slot[0])
        out[0, 0, :, columns(lax.rem(my_tp + n_tp - p, n_tp), 0)] = found

    all_fan().wait_send()
    all_early().wait_send()
    ep_sent().wait_send()
    blocks = (chunks - 1) * (n_tp - 1)

    @pl.when(others)
    def _():
        all_tp(blocks).wait()

    @pl.when(mid)
    def _():
        all_tp(blocks - most).wait()

    for p in range(most):
        pl.when(jnp.logical_and(mid, p >= keep))(
            to_tp(chunks - 1 - p, across, late_send.at[p], late_recv.at[p]).wait)


def writer(saved, out, token, sem):
    pieces = sem.shape[0]
    rows = saved.shape[2] // pieces
    copies = [
        pltpu.make_async_copy(
            saved.at[0, 0, pl.ds(p * rows, rows)], out.at[0, 0, pl.ds(p * rows, rows)], sem.at[p])
        for p in range(pieces)
    ]
    for copy in copies:
        copy.start()
    for copy in copies:
        copy.wait()
    token[...] = jnp.zeros_like(token)


def write_out(saved):
    tiles = max(saved.shape[2] // SUBLANES, 1)
    pieces = max(p for p in range(1, WRITES + 1) if tiles % p == 0)
    return pl.pallas_call(
        writer,
        out_shape=(jax.ShapeDtypeStruct(saved.shape, saved.dtype), pltpu.VMEM((8, LANES), jnp.float32)),
        in_specs=[pl.BlockSpec(memory_space=pltpu.VMEM)],
        out_specs=(pl.BlockSpec(memory_space=pl.ANY), pl.BlockSpec(memory_space=pltpu.VMEM)),
        scratch_shapes=[pltpu.SemaphoreType.DMA((pieces,))],
        compiler_params=pltpu.CompilerParams(vmem_limit_bytes=SPARE),
    )(saved)


def swap(n_tp, chunk, kept, token, got, send_sem, recv_sem):
    del token
    my_tp = lax.axis_index("tp")
    other = n_tp - 1 - my_tp
    most = kept.shape[1] // chunk
    keep = kept_by(lax.axis_index("dp"), most)

    @pl.when(middle_of(my_tp, n_tp))
    def _():
        barrier = pltpu.get_barrier_semaphore()
        pl.semaphore_signal(barrier, inc=1, device_id={"tp": other}, device_id_type=MESH)
        pl.semaphore_wait(barrier, 1)
        for count in kept_counts(most):
            part = pl.ds((most - count) * chunk, count * chunk)
            copy = pltpu.make_async_remote_copy(
                kept.at[:, part], got.at[:, part], send_sem, recv_sem,
                device_id={"tp": other}, device_id_type=MESH)
            pl.when(keep == count)(copy.start)
        for count in kept_counts(most):
            part = pl.ds((most - count) * chunk, count * chunk)
            copy = pltpu.make_async_remote_copy(
                kept.at[:, part], got.at[:, part], send_sem, recv_sem,
                device_id={"tp": other}, device_id_type=MESH)
            pl.when(keep == count)(copy.wait)


def exchange(n_tp, chunk, kept, token):
    return pl.pallas_call(
        functools.partial(swap, n_tp, chunk),
        out_shape=pltpu.VMEM(kept.shape, kept.dtype),
        in_specs=[pl.BlockSpec(memory_space=pltpu.VMEM)] * 2,
        out_specs=pl.BlockSpec(memory_space=pltpu.VMEM),
        scratch_shapes=[pltpu.SemaphoreType.DMA, pltpu.SemaphoreType.DMA],
        compiler_params=pltpu.CompilerParams(collective_id=1, has_side_effects=True, vmem_limit_bytes=SPARE),
    )(kept, token)


def finish(n_tp, hidden, chunk, got, written, out, sem):
    del written
    my_tp = lax.axis_index("tp")
    most = got.shape[1] // chunk
    keep = kept_by(lax.axis_index("dp"), most)
    end = (n_tp - my_tp) * hidden

    @pl.when(middle_of(my_tp, n_tp))
    def _():
        for count in kept_counts(most):
            size = count * chunk
            copy = pltpu.make_async_copy(
                got.at[:, pl.ds((most - count) * chunk, size)],
                out.at[0, 0, :, pl.ds(pl.multiple_of(end - size, chunk), size)], sem)

            @pl.when(keep == count)
            def _():
                copy.start()
                copy.wait()


def write_rest(n_tp, hidden, chunk, got, written):
    return pl.pallas_call(
        functools.partial(finish, n_tp, hidden, chunk),
        out_shape=jax.ShapeDtypeStruct(written.shape, written.dtype),
        in_specs=[pl.BlockSpec(memory_space=pltpu.VMEM), pl.BlockSpec(memory_space=pl.ANY)],
        out_specs=pl.BlockSpec(memory_space=pl.ANY),
        scratch_shapes=[pltpu.SemaphoreType.DMA],
        input_output_aliases={1: 0},
        compiler_params=pltpu.CompilerParams(vmem_limit_bytes=SPARE),
    )(got, written)


def local(down_weight, owned_span):
    n_ep, n_tp, n_dp = (lax.axis_size(a) for a in ("ep", "tp", "dp"))
    _, hidden, width = down_weight.shape
    rows = width // n_tp
    chunk = min(CHUNK, hidden)
    chunks = hidden // chunk
    most = min(max(KEEP), chunks - 1)
    kind = down_weight.dtype
    results = (n_tp * hidden + most * chunk) * rows * kind.itemsize
    saved, kept = pl.pallas_call(
        functools.partial(kernel, n_ep, n_tp, n_dp, chunk, most),
        out_shape=(pltpu.VMEM((1, 1, rows, n_tp * hidden), kind), pltpu.VMEM((rows, most * chunk), kind)),
        in_specs=[pl.BlockSpec(memory_space=pl.ANY), pl.BlockSpec(memory_space=pl.ANY)],
        out_specs=(pl.BlockSpec(memory_space=pltpu.VMEM), pl.BlockSpec(memory_space=pltpu.VMEM)),
        scratch_shapes=[
            pltpu.VMEM((STAGES, chunk, width), kind),
            pltpu.VMEM((width, chunk), kind),
            pltpu.VMEM(((chunks - 1) * (n_ep - 1), rows, chunk), kind),
            pltpu.VMEM(((chunks - 1) * (n_tp - 1), rows, chunk), kind),
            pltpu.SMEM((n_ep, n_dp, n_tp), jnp.int32),
            pltpu.VMEM((n_tp - 1, rows, chunk), kind),
            pltpu.VMEM((n_tp, rows, chunk), kind),
            pltpu.VMEM((n_ep - 1, n_tp, rows, chunk), kind),
            pltpu.SemaphoreType.DMA((STAGES,)),
            pltpu.SemaphoreType.DMA,
            pltpu.SemaphoreType.DMA,
            pltpu.SemaphoreType.DMA((chunks - 1,)),
            pltpu.SemaphoreType.DMA,
            pltpu.SemaphoreType.DMA,
            pltpu.SemaphoreType.DMA((most,)),
            pltpu.SemaphoreType.DMA((most,)),
            pltpu.SemaphoreType.DMA,
            pltpu.SemaphoreType.DMA,
            pltpu.SemaphoreType.DMA,
            pltpu.SemaphoreType.DMA,
            pltpu.SemaphoreType.REGULAR,
            pltpu.SemaphoreType.REGULAR,
        ] + [pltpu.VMEM((n_ep, rows, chunk), kind) for _ in range(chunks - 1)],
        compiler_params=pltpu.CompilerParams(
            collective_id=0, has_side_effects=True, vmem_limit_bytes=VMEM_BYTES - results),
    )(down_weight, jnp.transpose(owned_span, (0, 2, 1)))
    written, token = write_out(saved)
    return write_rest(n_tp, hidden, chunk, exchange(n_tp, chunk, kept, token), written)


def solution(mesh):
    return jax.shard_map(
        local,
        mesh=mesh,
        in_specs=(P("ep", "tp", "dp"), P()),
        out_specs=P("ep", "tp", "dp", None),
        check_vma=False,
    )
```

```python
import functools

import jax
import jax.numpy as jnp
from jax import lax
from jax.experimental import pallas as pl
from jax.experimental.pallas import tpu as pltpu
from jax.sharding import PartitionSpec as P

MESH = pl.DeviceIdType.MESH
LANES = 128
SUBLANES = 16
CHUNK = 256
STAGES = 4
AHEAD = 2
SPARE = 3 << 20
VMEM_BYTES = 67043328
WRITES = 8
KEEP = (1, 4)


def pick(values, index):
    chosen = values[0]
    for b in range(1, len(values)):
        chosen = jnp.where(index == b, values[b], chosen)
    return chosen


def middle_of(my_tp, n_tp):
    return jnp.logical_or(my_tp == n_tp // 2 - 1, my_tp == n_tp // 2)


def kept_by(my_dp, most):
    return jnp.where(my_dp % 2 == 0, min(KEEP[0], most), min(KEEP[1], most))


def kept_counts(most):
    return sorted({min(k, most) for k in KEEP})


def kernel(n_ep, n_tp, n_dp, chunk, most, weight, span_hbm, out, kept, stage, turned, send, relay, span,
           early, middle, spread, load_sem, span_sem, ep_send, ep_recv, tp_send, tp_recv, late_send, late_recv,
           early_send, early_recv, fan_send, fan_recv, settled, ready, *arrived):
    my_ep = lax.axis_index("ep")
    my_tp = lax.axis_index("tp")
    my_dp = lax.axis_index("dp")
    hidden, width = weight.shape[1], weight.shape[2]
    rows = width // n_tp
    chunks = hidden // chunk
    per_expert = n_tp * n_dp
    keep = kept_by(my_dp, most)
    mid = middle_of(my_tp, n_tp)
    others = jnp.logical_not(mid)

    near = my_tp < n_tp // 2
    edge = jnp.where(near, my_tp, n_tp - 1 - my_tp)
    ways = []
    for k in range(n_tp - 1):
        m = k - (n_tp - 1 - 2 * edge)
        step = edge - jnp.maximum(m, 0) // 2
        inner = jnp.where(jnp.maximum(m, 0) % 2 == 0, step, n_tp - step)
        hop = jnp.where(m < 0, n_tp - 1 - edge - k, inner)
        ways.append(jnp.where(near, hop, n_tp - hop))
    across = n_tp - 3

    def load(c):
        return pltpu.make_async_copy(
            weight.at[0, pl.ds(c * chunk, chunk)], stage.at[c % STAGES], load_sem.at[c % STAGES])

    half = chunk // 2

    def first_load(h):
        part = pl.ds(h * half, half)
        return pltpu.make_async_copy(weight.at[0, part], stage.at[0, part], load_sem.at[h * STAGES])

    def remote(src, dst, send_sem, recv_sem, axis, d, n):
        me = my_ep if axis == "ep" else my_tp
        return pltpu.make_async_remote_copy(
            src, dst, send_sem, recv_sem, device_id={axis: lax.rem(me + d, n)}, device_id_type=MESH)

    def to_ep(c, d):
        return remote(send.at[(c - 1) * (n_ep - 1) + d - 1], arrived[c - 1].at[d], ep_send, ep_recv.at[c - 1], "ep", d, n_ep)

    def columns(tp, c):
        return pl.ds(pl.multiple_of(tp * hidden + c * chunk, chunk), chunk)

    def to_tp(c, k, send_sem, recv_sem):
        return remote(
            relay.at[(c - 1) * (n_tp - 1) + k], out.at[0, 0, :, columns(my_tp, c)], send_sem, recv_sem, "tp", ways[k], n_tp)

    def early_to_tp(k):
        return remote(early.at[k], middle.at[ways[k]], early_send, early_recv, "tp", ways[k], n_tp)

    def fan(d):
        return remote(middle, spread.at[d - 1], fan_send, fan_recv, "ep", d, n_ep)

    def ep_sent():
        return remote(send, send, ep_send, ep_recv.at[0], "ep", 1, n_ep)

    def ep_got(c):
        here = arrived[c - 1].at[pl.ds(1, n_ep - 1)]
        return remote(here, here, ep_send, ep_recv.at[c - 1], "ep", 1, n_ep)

    def all_tp(blocks):
        return remote(
            relay.at[pl.ds(0, blocks)], out.at[0, 0, :, pl.ds(0, blocks * chunk)], tp_send, tp_recv, "tp", 1, n_tp)

    def all_early():
        return remote(early, middle.at[pl.ds(1, n_tp - 1)], early_send, early_recv, "tp", 1, n_tp)

    def all_fan():
        return remote(spread, spread, fan_send, fan_recv, "ep", 1, n_ep)

    first_load(0).start()
    first_load(1).start()
    barrier = pltpu.get_barrier_semaphore()

    def tell(sem, axis, index):
        pl.semaphore_signal(sem, inc=1, device_id={axis: index}, device_id_type=MESH)

    ep_peers = [lax.rem(my_ep + d, n_ep) for d in range(n_ep - 1, 0, -1)]
    tp_peers = [lax.rem(my_tp + d, n_tp) for d in range(1, n_tp)]

    @pl.when(mid)
    def _():
        tell(barrier, "tp", n_tp - 1 - my_tp)

    @pl.when(others)
    def _():
        for peer in tp_peers:
            pl.when(jnp.logical_not(middle_of(peer, n_tp)))(functools.partial(tell, barrier, "tp", peer))
        for peer in ep_peers:
            tell(barrier, "ep", peer)

    span_copy = pltpu.make_async_copy(span_hbm, span, span_sem)
    span_copy.start()
    span_copy.wait()

    def block_here(g):
        return jnp.where(lax.div(g, per_expert) == my_ep, lax.rem(g, per_expert) - my_dp * n_tp, 0)

    def sooner(d):
        j = lax.rem(my_tp + d, n_tp)
        return sum((block_here(span[i, my_dp, j]) for i in range(n_ep)), jnp.int32(0))

    def turn(c):
        if c == 0:
            first_load(0).wait()
            first_load(1).wait()
        else:
            load(c).wait()

        @pl.loop(0, width // LANES)
        def _(b):
            at = pl.multiple_of(b * LANES, LANES)
            turned[pl.ds(at, LANES), :] = stage[c % STAGES, :, pl.ds(at, LANES)].T

        if c + STAGES < chunks:
            load(c + STAGES).start()

    def block_of(index):
        return pick([turned[b * rows:(b + 1) * rows, :] for b in range(n_tp)], index)

    def first_block(target, index):
        if rows % LANES:
            target[...] = block_of(index)
            return
        for q in range(0, rows, LANES):
            tiles = [stage[0, :, b * rows + q:b * rows + q + LANES] for b in range(n_tp)]
            target[q:q + LANES, :] = pick(tiles, index).T

    def first_half(c):
        if c > 1:
            turn(c)
        for d in range(n_ep - 1, -1, -1):
            if d == 0:
                arrived[c - 1][0] = block_of(wanted[d])
            else:
                send[(c - 1) * (n_ep - 1) + d - 1] = block_of(wanted[d])
                to_ep(c, d).start()

    def second_half(c):
        ep_got(c).wait_recv()
        p = chunks - 1 - c
        for k in range(n_tp - 1):
            piece = pick([arrived[c - 1][s] for s in range(n_ep)], slot[k + 1])
            relay[(c - 1) * (n_tp - 1) + k] = piece
            if k == across and p < most:
                kept[:, (most - 1 - p) * chunk:(most - p) * chunk] = piece
                pl.when(others)(to_tp(c, k, tp_send, tp_recv).start)
                pl.when(jnp.logical_and(mid, p >= keep))(to_tp(c, k, late_send.at[p], late_recv.at[p]).start)
            else:
                to_tp(c, k, tp_send, tp_recv).start()
        out[0, 0, :, columns(my_tp, c)] = pick([arrived[c - 1][s] for s in range(n_ep)], slot[0])

    halves = rows % LANES == 0 and half % LANES == 0
    if rows % LANES:
        turn(0)
    else:
        first_load(0).wait()
        if not halves:
            first_load(1).wait()
    def start_loads():
        for later in range(1, min(STAGES, chunks)):
            load(later).start()

    later_places = [k for k in range(n_tp - 1) if k != across]

    @pl.when(mid)
    def _():
        if halves:
            index = sooner(ways[across])
            for h in range(2):
                part = pl.ds(h * half, half)
                if h:
                    first_load(1).wait()
                for q in range(0, rows, LANES):
                    tiles = [stage[0, h * half:(h + 1) * half, b * rows + q:b * rows + q + LANES] for b in range(n_tp)]
                    early[across, q:q + LANES, h * half:(h + 1) * half] = pick(tiles, index).T
                if h == 0:
                    pl.semaphore_wait(barrier, 1)
                remote(
                    early.at[across, :, part], middle.at[ways[across], :, part], early_send, early_recv,
                    "tp", ways[across], n_tp).start()
        else:
            first_block(early.at[across], sooner(ways[across]))
            pl.semaphore_wait(barrier, 1)
            early_to_tp(across).start()
        start_loads()
        for peer in tp_peers:
            pl.when(jnp.logical_not(middle_of(peer, n_tp)))(functools.partial(tell, barrier, "tp", peer))
        for k in later_places:
            first_block(early.at[k], sooner(ways[k]))
        first_block(middle.at[0], sooner(0))

    @pl.when(others)
    def _():
        if halves:
            first_load(1).wait()
        start_loads()
        for k in range(n_tp - 1):
            first_block(early.at[k], sooner(ways[k]))
        first_block(middle.at[0], sooner(0))
        pl.semaphore_wait(barrier, n_ep + n_tp - 2)
        for peer in ep_peers:
            tell(settled, "ep", peer)
        for k in range(n_tp - 1):
            early_to_tp(k).start()

    if rows % LANES == 0 and STAGES < chunks:
        load(STAGES).start()
    turn(1)

    wanted = []
    for d in range(n_ep):
        i = lax.rem(my_ep + d, n_ep)
        wanted.append(sum((block_here(span[i, my_dp, j]) for j in range(n_tp)), jnp.int32(0)))
    slot = []
    for d in [0] + ways:
        j = lax.rem(my_tp + d, n_tp)
        slot.append(lax.rem(my_ep + n_ep - lax.div(span[my_ep, my_dp, j], per_expert), n_ep))

    @pl.when(others)
    def _():
        pl.semaphore_wait(settled, n_ep - 1)
        for peer in tp_peers:
            pl.when(middle_of(peer, n_tp))(functools.partial(tell, ready, "tp", peer))

    @pl.when(mid)
    def _():
        pl.semaphore_wait(ready, n_tp - 2)
        for k in later_places:
            early_to_tp(k).start()

    for step in range(1, chunks + AHEAD):
        if step < chunks:
            first_half(step)
        if step == chunks:
            all_early().wait_recv()
            for d in range(1, n_ep):
                fan(d).start()
        if step > AHEAD:
            second_half(step - AHEAD)

    all_fan().wait_recv()
    for p in range(n_tp):
        found = pick([middle[p]] + [spread[d - 1, p] for d in range(1, n_ep)], slot[0])
        out[0, 0, :, columns(lax.rem(my_tp + n_tp - p, n_tp), 0)] = found

    all_fan().wait_send()
    all_early().wait_send()
    ep_sent().wait_send()
    blocks = (chunks - 1) * (n_tp - 1)

    @pl.when(others)
    def _():
        all_tp(blocks).wait()

    @pl.when(mid)
    def _():
        all_tp(blocks - most).wait()

    for p in range(most):
        pl.when(jnp.logical_and(mid, p >= keep))(
            to_tp(chunks - 1 - p, across, late_send.at[p], late_recv.at[p]).wait)


def writer(saved, out, token, sem):
    pieces = sem.shape[0]
    rows = saved.shape[2] // pieces
    copies = [
        pltpu.make_async_copy(
            saved.at[0, 0, pl.ds(p * rows, rows)], out.at[0, 0, pl.ds(p * rows, rows)], sem.at[p])
        for p in range(pieces)
    ]
    for copy in copies:
        copy.start()
    for copy in copies:
        copy.wait()
    token[...] = jnp.zeros_like(token)


def write_out(saved):
    tiles = max(saved.shape[2] // SUBLANES, 1)
    pieces = max(p for p in range(1, WRITES + 1) if tiles % p == 0)
    return pl.pallas_call(
        writer,
        out_shape=(jax.ShapeDtypeStruct(saved.shape, saved.dtype), pltpu.VMEM((8, LANES), jnp.float32)),
        in_specs=[pl.BlockSpec(memory_space=pltpu.VMEM)],
        out_specs=(pl.BlockSpec(memory_space=pl.ANY), pl.BlockSpec(memory_space=pltpu.VMEM)),
        scratch_shapes=[pltpu.SemaphoreType.DMA((pieces,))],
        compiler_params=pltpu.CompilerParams(vmem_limit_bytes=SPARE),
    )(saved)


def swap(n_tp, chunk, kept, token, got, send_sem, recv_sem):
    del token
    my_tp = lax.axis_index("tp")
    other = n_tp - 1 - my_tp
    most = kept.shape[1] // chunk
    keep = kept_by(lax.axis_index("dp"), most)

    @pl.when(middle_of(my_tp, n_tp))
    def _():
        barrier = pltpu.get_barrier_semaphore()
        pl.semaphore_signal(barrier, inc=1, device_id={"tp": other}, device_id_type=MESH)
        pl.semaphore_wait(barrier, 1)
        for count in kept_counts(most):
            part = pl.ds((most - count) * chunk, count * chunk)
            copy = pltpu.make_async_remote_copy(
                kept.at[:, part], got.at[:, part], send_sem, recv_sem,
                device_id={"tp": other}, device_id_type=MESH)
            pl.when(keep == count)(copy.start)
        for count in kept_counts(most):
            part = pl.ds((most - count) * chunk, count * chunk)
            copy = pltpu.make_async_remote_copy(
                kept.at[:, part], got.at[:, part], send_sem, recv_sem,
                device_id={"tp": other}, device_id_type=MESH)
            pl.when(keep == count)(copy.wait)


def exchange(n_tp, chunk, kept, token):
    return pl.pallas_call(
        functools.partial(swap, n_tp, chunk),
        out_shape=pltpu.VMEM(kept.shape, kept.dtype),
        in_specs=[pl.BlockSpec(memory_space=pltpu.VMEM)] * 2,
        out_specs=pl.BlockSpec(memory_space=pltpu.VMEM),
        scratch_shapes=[pltpu.SemaphoreType.DMA, pltpu.SemaphoreType.DMA],
        compiler_params=pltpu.CompilerParams(collective_id=1, has_side_effects=True, vmem_limit_bytes=SPARE),
    )(kept, token)


def finish(n_tp, hidden, chunk, got, written, out, sem):
    del written
    my_tp = lax.axis_index("tp")
    most = got.shape[1] // chunk
    keep = kept_by(lax.axis_index("dp"), most)
    end = (n_tp - my_tp) * hidden

    @pl.when(middle_of(my_tp, n_tp))
    def _():
        for count in kept_counts(most):
            size = count * chunk
            copy = pltpu.make_async_copy(
                got.at[:, pl.ds((most - count) * chunk, size)],
                out.at[0, 0, :, pl.ds(pl.multiple_of(end - size, chunk), size)], sem)

            @pl.when(keep == count)
            def _():
                copy.start()
                copy.wait()


def write_rest(n_tp, hidden, chunk, got, written):
    return pl.pallas_call(
        functools.partial(finish, n_tp, hidden, chunk),
        out_shape=jax.ShapeDtypeStruct(written.shape, written.dtype),
        in_specs=[pl.BlockSpec(memory_space=pltpu.VMEM), pl.BlockSpec(memory_space=pl.ANY)],
        out_specs=pl.BlockSpec(memory_space=pl.ANY),
        scratch_shapes=[pltpu.SemaphoreType.DMA],
        input_output_aliases={1: 0},
        compiler_params=pltpu.CompilerParams(vmem_limit_bytes=SPARE),
    )(got, written)


def local(down_weight, owned_span):
    n_ep, n_tp, n_dp = (lax.axis_size(a) for a in ("ep", "tp", "dp"))
    _, hidden, width = down_weight.shape
    rows = width // n_tp
    chunk = min(CHUNK, hidden)
    chunks = hidden // chunk
    most = min(max(KEEP), chunks - 1)
    kind = down_weight.dtype
    results = (n_tp * hidden + most * chunk) * rows * kind.itemsize
    saved, kept = pl.pallas_call(
        functools.partial(kernel, n_ep, n_tp, n_dp, chunk, most),
        out_shape=(pltpu.VMEM((1, 1, rows, n_tp * hidden), kind), pltpu.VMEM((rows, most * chunk), kind)),
        in_specs=[pl.BlockSpec(memory_space=pl.ANY), pl.BlockSpec(memory_space=pl.ANY)],
        out_specs=(pl.BlockSpec(memory_space=pltpu.VMEM), pl.BlockSpec(memory_space=pltpu.VMEM)),
        scratch_shapes=[
            pltpu.VMEM((STAGES, chunk, width), kind),
            pltpu.VMEM((width, chunk), kind),
            pltpu.VMEM(((chunks - 1) * (n_ep - 1), rows, chunk), kind),
            pltpu.VMEM(((chunks - 1) * (n_tp - 1), rows, chunk), kind),
            pltpu.SMEM((n_ep, n_dp, n_tp), jnp.int32),
            pltpu.VMEM((n_tp - 1, rows, chunk), kind),
            pltpu.VMEM((n_tp, rows, chunk), kind),
            pltpu.VMEM((n_ep - 1, n_tp, rows, chunk), kind),
            pltpu.SemaphoreType.DMA((STAGES + 1,)),
            pltpu.SemaphoreType.DMA,
            pltpu.SemaphoreType.DMA,
            pltpu.SemaphoreType.DMA((chunks - 1,)),
            pltpu.SemaphoreType.DMA,
            pltpu.SemaphoreType.DMA,
            pltpu.SemaphoreType.DMA((most,)),
            pltpu.SemaphoreType.DMA((most,)),
            pltpu.SemaphoreType.DMA,
            pltpu.SemaphoreType.DMA,
            pltpu.SemaphoreType.DMA,
            pltpu.SemaphoreType.DMA,
            pltpu.SemaphoreType.REGULAR,
            pltpu.SemaphoreType.REGULAR,
        ] + [pltpu.VMEM((n_ep, rows, chunk), kind) for _ in range(chunks - 1)],
        compiler_params=pltpu.CompilerParams(
            collective_id=0, has_side_effects=True, vmem_limit_bytes=VMEM_BYTES - results),
    )(down_weight, jnp.transpose(owned_span, (0, 2, 1)))
    written, token = write_out(saved)
    return write_rest(n_tp, hidden, chunk, exchange(n_tp, chunk, kept, token), written)


def solution(mesh):
    return jax.shard_map(
        local,
        mesh=mesh,
        in_specs=(P("ep", "tp", "dp"), P()),
        out_specs=P("ep", "tp", "dp", None),
        check_vma=False,
    )
```
